32 devices in a mesh: dp: 2 (over y), seq: 16 (over z, x, core).
Axes of the slice: x: 2, y: 2, z: 4, core: 2. Of those that a mesh axis runs over, the one named last changes fastest.
Arguments:
- hidden_in: bfloat16 [2, 1024, 2048], P('dp', 'seq'), may hold values from -6 to 6
- attn_gain: float32 [2048], replicated, may hold values from 0.1 to 1.9
- w_query: bfloat16 [2048, 1280], P('dp'), may hold values from -2 to 2
- w_keyval: bfloat16 [2048, 512], P('dp'), may hold values from -1 to 1
- w_output: bfloat16 [1280, 2048], P(None, 'dp'), may hold values from -0.15625 to 0.15625
- post_gain: float32 [2048], replicated, may hold values from 0.1 to 1.9
Outputs:
- hidden_out: bfloat16 [2, 1024, 2048], P('dp', 'seq')
The draws below stay inside these ranges and needn't reach their ends.
All inputs are finite; a program needn't handle non-finite values.
Results may differ from the reference program's by a relative error of at most 0.009.
Values may be sent and summed in bfloat16 or wider, within the bound.
No kernel may reach another device: no remote copies, remote signals or barrier semaphores. Data moves between devices by JAX's collectives and lax.ppermute only.
A program may use at most 64 MiB of HBM per device.

```python
import jax
import jax.numpy as jnp
from jax import lax

D = 2048
HEADS = 5
HD = 256
EPISODES = 2
SEQLEN = 1024


def key_columns(key):
    return jax.random.truncated_normal(jax.random.fold_in(key, 11), -4.0, 4.0, (D, HD), jnp.float32) / jnp.sqrt(jnp.float32(D))


def draw_w_keyval(key, part):
    values = jax.random.truncated_normal(jax.random.fold_in(key, 12), -4.0, 4.0, (D, HD), jnp.float32) / jnp.sqrt(jnp.float32(D))
    return jnp.concatenate([key_columns(key), values], axis=1).astype(jnp.bfloat16)


def draw_w_query(key, part):
    noise = jax.random.truncated_normal(jax.random.fold_in(key, 13), -4.0, 4.0, (D, HEADS, HD), jnp.float32) / jnp.sqrt(jnp.float32(D))
    result = noise
    return result.reshape(D, HEADS * HD).astype(jnp.bfloat16)


def block_scale(own_key, dims, split, least, high):
    def one(axis_at, blocks):
        draws = jax.random.uniform(jax.random.fold_in(jax.random.fold_in(own_key, 6), axis_at), (blocks,), jnp.float32, least / len(split), high / len(split))
        return jnp.repeat(jnp.exp(draws), dims[axis_at] // blocks).reshape((-1,) + (1,) * (len(dims) - axis_at - 1))

    factor_of = one(*split[0])
    for cut in split[1:]:
        factor_of = factor_of * one(*cut)
    return factor_of


def bell_draw(stream_key, dims, scale, bound, shards=(), kind=jnp.bfloat16):
    values = scale * jax.random.normal(stream_key, dims, jnp.float32)
    if shards:
        values = values * block_scale(stream_key, dims, shards, -0.22, 0.18)
    return jnp.clip(values, -bound, bound).astype(kind)


def setup_inputs(seed: int = 0) -> dict:
    key_of = jax.random.split(jax.random.key(seed), 7)
    hidden_in = bell_draw(key_of[0], (EPISODES, SEQLEN, D), 1.0, 6.0, ((0, 2), (1, 16)))
    attn_gain = jnp.clip(1.0 + 0.18 * jax.random.normal(key_of[1], (D,), jnp.float32), 0.1, 1.9)
    w_query = draw_w_query(jax.random.fold_in(key_of[6], 71), 0)
    w_keyval = draw_w_keyval(jax.random.fold_in(key_of[6], 71), 0)
    w_output = bell_draw(key_of[4], (HEADS * HD, D), (HEADS * HD) ** -0.5, 0.15625, ((1, 2),))
    post_gain = jnp.clip(1.0 + 0.18 * jax.random.normal(key_of[5], (D,), jnp.float32), 0.1, 1.9)
    return dict(hidden_in=hidden_in, attn_gain=attn_gain, w_query=w_query, w_keyval=w_keyval, w_output=w_output, post_gain=post_gain)


def rms_norm(v, gain):
    v = v.astype(jnp.float32)
    return v * lax.rsqrt(lax.optimization_barrier(jnp.mean(v * v, axis=-1, keepdims=True)) + 1e-06) * gain

def rotary(t, positions):
    half = t.shape[-1] // 2
    freq = jnp.exp(-jnp.log(10000.0) * jnp.arange(half, dtype=jnp.float32) * 2.0 / t.shape[-1])
    angle = positions.astype(jnp.float32)[:, None, None] * freq[None, None, :]
    cosine = jnp.cos(angle)
    sine = jnp.sin(angle)
    first = t[..., :half]
    second = t[..., half:]
    return jnp.concatenate([first * cosine - second * sine, second * cosine + first * sine], axis=-1)

def reference(hidden_in, attn_gain, w_query, w_keyval, w_output, post_gain):

    def episode(frame):
        normed = rms_norm(frame, attn_gain).astype(jnp.bfloat16)
        query_raw = jnp.dot(normed, w_query, preferred_element_type=jnp.float32)
        keyval_raw = jnp.dot(normed, w_keyval, preferred_element_type=jnp.float32)
        positions = jnp.arange(SEQLEN, dtype=jnp.int32)
        query = (rotary(query_raw.reshape(SEQLEN, HEADS, HD), positions) * HD ** (-0.5)).astype(jnp.bfloat16)
        keys = rotary(keyval_raw[:, None, :HD], positions)[:, 0, :].astype(jnp.bfloat16)
        values = keyval_raw[:, HD:].astype(jnp.bfloat16)

        def one_head(query_head):
            scores = jnp.dot(query_head, keys.T, preferred_element_type=jnp.float32)
            rowmax = lax.optimization_barrier(jnp.max(scores, axis=1, keepdims=True))
            expo = jnp.exp(scores - rowmax)
            total = lax.optimization_barrier(jnp.sum(expo, axis=1, keepdims=True))
            summed = jnp.dot(expo.astype(jnp.bfloat16), values, preferred_element_type=jnp.float32)
            return summed / total
        heads = lax.map(one_head, jnp.transpose(query, (1, 0, 2)))
        attended = jnp.transpose(heads, (1, 0, 2)).reshape(SEQLEN, HEADS * HD).astype(jnp.bfloat16)
        projected = jnp.dot(attended, w_output, preferred_element_type=jnp.float32)
        return (frame.astype(jnp.float32) + rms_norm(projected, post_gain)).astype(jnp.bfloat16)
    return lax.map(episode, hidden_in)
```

```python
import jax
import jax.numpy as jnp
from jax import lax
from jax.sharding import PartitionSpec as P


def shift(v, axis, k, n):
    return lax.ppermute(v, axis, [(i, (i + k) % n) for i in range(n)])


def partner(v, axis, k, n):
    return lax.ppermute(v, axis, [(i, i ^ k) for i in range(n)])


def rotate(first, second, cosine, sine):
    return first * cosine - second * sine, second * cosine + first * sine


def gather_rows(v, axis, n):
    if n & (n - 1):
        return lax.all_gather(v, axis, axis=0, tiled=True)
    near = min(4, n)
    pieces = [v] + [partner(v, axis, k, n) for k in range(near, n, near)]
    whole = jnp.concatenate(pieces, axis=0)
    step = near // 2
    while step:
        whole = jnp.concatenate([whole, partner(whole, axis, step, n)], axis=0)
        step //= 2
    return whole


def make_local(dp, seq):
    def local(hidden_in, attn_gain, w_query, w_keyval, w_output, post_gain):
        frame = hidden_in[0]
        count, width = frame.shape
        head_dim = w_keyval.shape[1] // 2
        half = head_dim // 2
        width_q = w_query.shape[1]
        num_heads = width_q // head_dim
        rows = w_query.shape[0]
        me = lax.axis_index("dp")
        seat = lax.axis_index("seq")

        def columns(v, who, axis):
            return lax.dynamic_slice_in_dim(v, who * rows, rows, axis)

        sent = [
            shift(columns(frame, lax.rem(me + k, dp), 1), "dp", k, dp) for k in range(1, dp)
        ]
        gain = columns(attn_gain, me, 0)[None, :]

        def scaled(v):
            return (v.astype(jnp.float32) * gain).astype(jnp.bfloat16)

        def dot(a, b):
            return jnp.dot(a, b, preferred_element_type=jnp.float32)

        own = scaled(columns(frame, me, 1))
        wide = frame.astype(jnp.float32)
        inverse = lax.rsqrt(jnp.mean(wide * wide, axis=-1, keepdims=True) + 1e-06)
        positions = seat * count + jnp.arange(count, dtype=jnp.int32)
        freq = jnp.exp(
            -jnp.log(10000.0) * jnp.arange(half, dtype=jnp.float32) * 2.0 / head_dim
        )
        angle = positions.astype(jnp.float32)[:, None] * freq[None, :]
        cosine = jnp.cos(angle)
        sine = jnp.sin(angle)

        theirs = [scaled(v) for v in sent]
        back_kv = [
            shift(dot(v, w_keyval), "dp", dp - k, dp) for k, v in enumerate(theirs, 1)
        ]
        back_q = [
            shift(dot(v, w_query), "dp", dp - k, dp) for k, v in enumerate(theirs, 1)
        ]
        keyval_raw = sum(back_kv, dot(own, w_keyval)) * inverse
        k1, k2 = rotate(keyval_raw[:, :half], keyval_raw[:, half:head_dim], cosine, sine)
        keyval = jnp.concatenate([k1, k2, keyval_raw[:, head_dim:]], axis=1).astype(jnp.bfloat16)
        keyval = gather_rows(keyval, "seq", seq)

        query_raw = sum(back_q, dot(own, w_query)) * (inverse * head_dim ** (-0.5))
        stacked = []
        for h in range(num_heads):
            part = query_raw[:, h * head_dim : (h + 1) * head_dim]
            stacked.append(
                jnp.concatenate(rotate(part[:, :half], part[:, half:], cosine, sine), axis=1)
            )
        query = jnp.concatenate(stacked, axis=0).astype(jnp.bfloat16)
        scores = lax.dot_general(
            query, keyval[:, :head_dim], (((1,), (1,)), ((), ())), preferred_element_type=jnp.float32
        )
        expo = jnp.exp(scores - jnp.max(scores, axis=1, keepdims=True))
        total = jnp.sum(expo, axis=1, keepdims=True)
        heads = dot(expo.astype(jnp.bfloat16), keyval[:, head_dim:]) / total
        heads = heads.astype(jnp.bfloat16)
        attended = jnp.concatenate(
            [heads[h * count : (h + 1) * count] for h in range(num_heads)], axis=1
        )

        mine = dot(attended, w_output).astype(jnp.bfloat16)
        others = [shift(attended, "dp", k, dp) for k in range(1, dp)]
        returned = [
            shift(dot(v, w_output).astype(jnp.bfloat16), "dp", dp - k, dp)
            for k, v in enumerate(others, 1)
        ]
        post = post_gain[None, :]
        cols = w_output.shape[1]
        blocks = jnp.stack([mine] + returned)
        projected = jnp.concatenate(
            [
                lax.dynamic_index_in_dim(blocks, lax.rem(j - me + dp, dp), 0, keepdims=False)
                for j in range(dp)
            ],
            axis=1,
        ).astype(jnp.float32)
        scale = lax.rsqrt(jnp.mean(projected * projected, axis=-1, keepdims=True) + 1e-06)
        return (wide + projected * scale * post).astype(jnp.bfloat16)[None]

    return local


def solution(mesh):
    in_specs = (P("dp", "seq", None), P(), P("dp", None), P("dp", None), P(None, "dp"), P())
    out_specs = P("dp", "seq", None)
    return jax.shard_map(
        make_local(mesh.shape["dp"], mesh.shape["seq"]),
        mesh=mesh,
        in_specs=in_specs,
        out_specs=out_specs,
        check_vma=False,
    )
```
